32 devices in a mesh: groups: 2 (over y), seq: 4 (over z), tensor: 2 (over x), sub: 2 (over core).
Axes of the slice: x: 2, y: 2, z: 4, core: 2. Of those that a mesh axis runs over, the one named last changes fastest.
Arguments:
- image_tokens: bfloat16 [2048, 3072], P(('groups', 'seq')), parts along dimension 0, may hold values from -6 to 6
- text_tokens: bfloat16 [256, 3072], P(('groups', 'seq')), parts along dimension 0, may hold values from -6 to 6
- timestep: int32 [2], P('groups'), parts along dimension 0, may hold values from 0 to 49
- text_length: int32 [2], P('groups'), parts along dimension 0, may hold values from 32 to 128
- time_table: bfloat16 [50, 3072], replicated, may hold values from -6 to 6
- mod_weight: bfloat16 [3072, 18432], P('seq', ('tensor', 'sub')), may hold values from -0.109375 to 0.109375
- qkv_image: bfloat16 [3072, 6144], P('seq', ('tensor', 'sub')), as said below
- qkv_text: bfloat16 [3072, 6144], P('seq', ('tensor', 'sub')), as said below
- norm_gain: float32 [2, 2, 16, 128], P(None, None, ('tensor', 'sub')), may hold values from 1 to 6
- proj_image: bfloat16 [2048, 3072], P(('tensor', 'sub'), 'seq'), may hold values from -0.125 to 0.125
- proj_text: bfloat16 [2048, 3072], P(('tensor', 'sub'), 'seq'), may hold values from -0.125 to 0.125
Outputs:
- image_out: bfloat16 [2048, 3072], P(('groups', 'seq'), ('tensor', 'sub')), parts along dimension 0
- text_out: bfloat16 [256, 3072], P(('groups', 'seq'), ('tensor', 'sub')), parts along dimension 0
The draws below stay inside these ranges and needn't reach their ends.
There are 2 independent parts, one for each index of `groups`. The reference program is written for one: setup_inputs(seed, part) draws one part's arguments, and reference() takes and returns one part's arrays. A program takes and returns all parts, laid end to end along the dimension named above; an argument that names none is the same for every part. Nothing has to cross between parts.
Inputs may be any that keep to these rules, and one draw needn't show every extreme that they name: `qkv_image`: entries of standard deviation about 1/sqrt(3072). `qkv_text`: entries of standard deviation about 1/sqrt(3072).
All inputs are finite; a program needn't handle non-finite values.
Results may differ from the reference program's by a relative error of at most 0.0085.
Values may be sent and summed in bfloat16 or wider, within the bound.
No kernel may reach another device: no remote copies, remote signals or barrier semaphores. Data moves between devices by JAX's collectives and lax.ppermute only.
A program may use at most 64 MiB of HBM per device.

```python
import jax
import jax.numpy as jnp
from jax import lax

D = 3072
HEADS = 16
HD = 128
STEPS = 50
IMAGE = 1024
TEXT = 128


def qkv_draw(key, salt):
    base = jax.random.truncated_normal(jax.random.fold_in(key, salt), -6.0, 6.0, (D, HEADS, 3, HD), jnp.float32) * float(D) ** (-0.5)
    return base.reshape(D, 3 * HEADS * HD)


def draw_qkv_image(key, part):
    return qkv_draw(key, 11).astype(jnp.bfloat16)


def draw_qkv_text(key, part):
    return qkv_draw(key, 13).astype(jnp.bfloat16)


def draw_norm_gain(key, part):
    logs = jax.random.uniform(jax.random.fold_in(key, 23), (2, 2, HEADS, HD), jnp.float32, jnp.log(1.2), jnp.log(3.0))
    result = jnp.exp(logs)
    return result.astype(jnp.float32)


def shard_levels(rng, shape, shards, low, high):
    loudness, own = 1.0, jax.random.fold_in(rng, 6)
    for axis_at, parts in shards:
        steps = jnp.exp(jax.random.uniform(jax.random.fold_in(own, axis_at), (parts,), jnp.float32, low / len(shards), high / len(shards)))
        loudness = loudness * jnp.repeat(steps, shape[axis_at] // parts).reshape([-1 if axis == axis_at else 1 for axis in range(len(shape))])
    return loudness


def normal_values(stream_key, extent, scale, reach, split=(), kind=jnp.bfloat16):
    values = scale * jax.random.normal(stream_key, extent, jnp.float32)
    if split:
        values = values * shard_levels(stream_key, extent, split, -0.22, 0.18)
    return jnp.clip(values, -reach, reach).astype(kind)


def setup_inputs(seed: int = 0, part: int = 0) -> dict:
    streams_of = jax.random.split(jax.random.key(seed), 12)
    part_keys = jax.random.split(jax.random.fold_in(streams_of[11], part), 12)
    return {
        "image_tokens": normal_values(part_keys[0], (IMAGE, D), 1.0, 6.0, ((0, 4),)),
        "text_tokens": normal_values(part_keys[1], (TEXT, D), 1.0, 6.0, ((0, 4),)),
        "timestep": jax.random.randint(part_keys[2], (1,), 0, STEPS).astype(jnp.int32),
        "text_length": jax.random.randint(part_keys[3], (1,), TEXT // 4, TEXT + 1).astype(jnp.int32),
        "time_table": normal_values(streams_of[4], (STEPS, D), 1.0, 6.0),
        "mod_weight": normal_values(streams_of[5], (D, 6 * D), D ** -0.5, 0.109375, ((0, 4), (1, 4))),
        "qkv_image": draw_qkv_image(jax.random.fold_in(streams_of[11], 71), part),
        "qkv_text": draw_qkv_text(jax.random.fold_in(streams_of[11], 71), part),
        "norm_gain": draw_norm_gain(jax.random.fold_in(streams_of[11], 71), part),
        "proj_image": normal_values(streams_of[9], (HEADS * HD, D), (HEADS * HD) ** -0.5, 0.125, ((0, 4), (1, 4))),
        "proj_text": normal_values(streams_of[10], (HEADS * HD, D), (HEADS * HD) ** -0.5, 0.125, ((0, 4), (1, 4))),
    }


EPSILON = 1e-06

def modulate(tokens, shift, scaling):
    values = tokens.astype(jnp.float32)
    center = lax.optimization_barrier(jnp.mean(values, axis=-1, keepdims=True))
    spread = lax.optimization_barrier(jnp.mean(jnp.square(values - center), axis=-1, keepdims=True))
    normed = (values - center) * lax.rsqrt(spread + EPSILON)
    return (normed * (1.0 + scaling) + shift).astype(jnp.bfloat16)

def head_norm(values, gain):
    return values * lax.rsqrt(lax.optimization_barrier(jnp.mean(values * values, axis=-1, keepdims=True)) + EPSILON) * gain

def split_heads(projected, gains):
    shaped = projected.reshape(projected.shape[0], -1, 3, gains.shape[-1])
    queries = head_norm(shaped[:, :, 0], gains[0]).astype(jnp.bfloat16)
    keys = head_norm(shaped[:, :, 1], gains[1]).astype(jnp.bfloat16)
    values = shaped[:, :, 2].astype(jnp.bfloat16)
    return (queries, keys, values)

def reference(image_tokens, text_tokens, timestep, text_length, time_table, mod_weight, qkv_image, qkv_text, norm_gain, proj_image, proj_text):
    embedded = lax.dynamic_index_in_dim(time_table, timestep[0], 0, keepdims=False).astype(jnp.float32)
    vector = jax.nn.silu(embedded).astype(jnp.bfloat16)
    modulation = jnp.dot(vector[None, :], mod_weight, preferred_element_type=jnp.float32)[0].reshape(2, 3, D)
    hidden_image = modulate(image_tokens, modulation[0, 0], modulation[0, 1])
    hidden_text = modulate(text_tokens, modulation[1, 0], modulation[1, 1])
    image_q, image_k, image_v = split_heads(jnp.dot(hidden_image, qkv_image, preferred_element_type=jnp.float32), norm_gain[0])
    text_q, text_k, text_v = split_heads(jnp.dot(hidden_text, qkv_text, preferred_element_type=jnp.float32), norm_gain[1])
    queries = jnp.concatenate([text_q, image_q], axis=0).transpose(1, 0, 2)
    keys = jnp.concatenate([text_k, image_k], axis=0).transpose(1, 0, 2)
    values = jnp.concatenate([text_v, image_v], axis=0).transpose(1, 0, 2)
    position = jnp.arange(TEXT + IMAGE, dtype=jnp.int32)
    usable = (position >= TEXT) | (position < text_length[0])
    factor = float(HD) ** (-0.5)

    def one_head(operands):
        head_q, head_k, head_v = operands
        scores = jnp.dot(head_q, head_k.T, preferred_element_type=jnp.float32) * factor
        scores = jnp.where(usable[None, :], scores, -1e+30)
        highest = lax.optimization_barrier(jnp.max(scores, axis=-1, keepdims=True))
        probs = jnp.exp(scores - highest)
        totals = lax.optimization_barrier(jnp.sum(probs, axis=-1, keepdims=True))
        mixed = jnp.dot(probs.astype(jnp.bfloat16), head_v, preferred_element_type=jnp.float32) / totals
        return mixed.astype(jnp.bfloat16)
    attended = lax.map(one_head, (queries, keys, values))
    attended = attended.transpose(1, 0, 2).reshape(TEXT + IMAGE, HEADS * HD)
    text_branch = jnp.dot(attended[:TEXT], proj_text, preferred_element_type=jnp.float32)
    image_branch = jnp.dot(attended[TEXT:], proj_image, preferred_element_type=jnp.float32)
    image_out = (image_tokens.astype(jnp.float32) + modulation[0, 2] * image_branch).astype(jnp.bfloat16)
    text_out = (text_tokens.astype(jnp.float32) + modulation[1, 2] * text_branch).astype(jnp.bfloat16)
    return (image_out, text_out)
```

```python
import functools

import jax
import jax.numpy as jnp
from jax import lax
from jax.experimental import pallas as pl
from jax.experimental.pallas import tpu as pltpu
from jax.sharding import PartitionSpec as P

EPSILON = 1e-06

VMEM = pl.BlockSpec(memory_space=pltpu.VMEM)
SMEM = pl.BlockSpec(memory_space=pltpu.SMEM)


def modulate(tokens, shift, scaling):
    values = tokens.astype(jnp.float32)
    center = jnp.mean(values, axis=-1, keepdims=True)
    spread = jnp.mean(jnp.square(values - center), axis=-1, keepdims=True)
    normed = (values - center) * lax.rsqrt(spread + EPSILON)
    return (normed * (1.0 + scaling) + shift).astype(jnp.bfloat16)


def head_norm(values, gain):
    return values * lax.rsqrt(jnp.mean(values * values, axis=-1, keepdims=True) + EPSILON) * gain


def mm(a, b):
    return jnp.dot(a, b, preferred_element_type=jnp.float32)


def qkv_kernel(pieces, index, *refs):
    tokens, (own, near, far, half, other, scale, shift, gain) = refs[:pieces], refs[pieces:-2]
    out, hidden = refs[-2:]
    rows = tokens[0].shape[0]
    step = 16
    factor = 1.0 + scale[...]
    offset = shift[...]
    for at, piece in enumerate(tokens):
        start = index[at] * rows if pieces > 1 else 0

        def body(i, carry, piece=piece, start=start):
            values = piece[pl.ds(pl.multiple_of(i * step, step), step), :].astype(jnp.float32)
            center = jnp.mean(values, axis=-1, keepdims=True)
            values = values - center
            spread = jnp.mean(values * values, axis=-1, keepdims=True)
            normed = values * lax.rsqrt(spread + EPSILON)
            hidden[pl.ds(pl.multiple_of(start + i * step, step), step), :] = (
                normed * factor + offset
            ).astype(jnp.bfloat16)
            return carry

        lax.fori_loop(0, rows // step, body, 0)

    slab = own.shape[0]

    def part(position, weights):
        depth = weights.shape[0]
        return mm(hidden[:, pl.ds(pl.multiple_of(position, 128), depth)], weights[...])

    total = part(index[4] * slab, own)
    total += part(index[5] * slab, near)
    total += part(index[6] * slab, far)
    total += part(index[7] * slab + index[8] * (slab // 2), half)
    total += part(index[7] * slab + index[9] * (slab // 2), other)
    size = gain.shape[1]
    out[:, :size] = head_norm(total[:, :size], gain[0:1, :]).astype(jnp.bfloat16)
    out[:, size : 2 * size] = head_norm(total[:, size : 2 * size], gain[1:2, :]).astype(
        jnp.bfloat16
    )
    out[:, 2 * size :] = total[:, 2 * size :].astype(jnp.bfloat16)


def attend_kernel(blocks, index, *refs):
    images, parts = refs[:blocks], refs[blocks : 2 * blocks]
    gain, out_image, out_text, keys, values, queries = refs[2 * blocks :]
    size = gain.shape[1]
    text = parts[0].shape[0]
    rows = images[0].shape[0]
    total = parts[0][...]
    for part in parts[1:]:
        total += part[...].astype(jnp.float32)
    queries[:text] = head_norm(total[:, :size], gain[0:1, :]).astype(jnp.bfloat16)
    keys[:text] = head_norm(total[:, size : 2 * size], gain[1:2, :]).astype(jnp.bfloat16)
    values[:text] = total[:, 2 * size :].astype(jnp.bfloat16)
    for at, image in enumerate(images):
        where = slice(text + at * rows, text + (at + 1) * rows)
        queries[where] = image[:, :size]
        keys[where] = image[:, size : 2 * size]
        values[where] = image[:, 2 * size :]
    length = index[0]
    factor = float(size) ** (-0.5)
    dims = (((1,), (1,)), ((), ()))
    step = 128

    def one(start):
        query = queries[pl.ds(start, step), :]
        lead = lax.dot_general(query, keys[:text], dims, preferred_element_type=jnp.float32)
        rest = lax.dot_general(query, keys[text:], dims, preferred_element_type=jnp.float32)
        lead, rest = lead * factor, rest * factor
        position = lax.broadcasted_iota(jnp.int32, lead.shape, 1)
        lead = jnp.where(position < length, lead, -1e30)
        highest = jnp.maximum(
            jnp.max(lead, axis=-1, keepdims=True), jnp.max(rest, axis=-1, keepdims=True)
        )
        lead, rest = jnp.exp(lead - highest), jnp.exp(rest - highest)
        sums = jnp.sum(lead, axis=-1, keepdims=True) + jnp.sum(rest, axis=-1, keepdims=True)
        mixed = mm(lead.astype(jnp.bfloat16), values[:text])
        mixed += mm(rest.astype(jnp.bfloat16), values[text:])
        return (mixed / sums).astype(jnp.bfloat16)

    for at in range(text // step):
        out_text[at * step : (at + 1) * step] = one(at * step)
    each = rows // step
    for at in range(blocks * each):
        block, inner = divmod(at, each)
        out_image[block, inner * step : (inner + 1) * step] = one(text + at * step)


def project_kernel(blocks, index, *refs):
    heads = refs[:blocks]
    own, near, far, half, other, out, joined = refs[blocks:]
    size = heads[0].shape[1]
    for at, head in enumerate(heads):
        joined[:, pl.ds(pl.multiple_of(index[at] * size, size), size)] = head[...]
    depth = own.shape[0] // 2
    whole = joined[...]
    out[index[4]] = mm(whole, own[...]).astype(jnp.bfloat16)
    out[index[5]] = mm(whole, near[...]).astype(jnp.bfloat16)
    out[index[6]] = mm(whole, far[...]).astype(jnp.bfloat16)
    first = joined[:, pl.ds(pl.multiple_of(index[8] * depth, depth), depth)]
    second = joined[:, pl.ds(pl.multiple_of(index[9] * depth, depth), depth)]
    out[index[7]] = (mm(first, half[...]) + mm(second, other[...])).astype(jnp.bfloat16)


def split_body(
    image_tokens,
    text_tokens,
    timestep,
    text_length,
    time_table,
    mod_weight,
    qkv_image,
    qkv_text,
    norm_gain,
    proj_image,
    proj_text,
):
    image_count, width = image_tokens.shape
    text_count = text_tokens.shape[0]
    seq = lax.axis_size("seq")
    tensor, sub = lax.axis_size("tensor"), lax.axis_size("sub")
    lanes = tensor * sub
    size = norm_gain.shape[3]
    slab = qkv_image.shape[0]
    across = qkv_image.shape[1] // seq
    y, z = lax.axis_index("groups"), lax.axis_index("seq")
    x, c = lax.axis_index("tensor"), lax.axis_index("sub")
    q = lax.axis_index(("tensor", "sub"))
    swap = [(0, 1), (1, 0)]

    def shift(value, by):
        return lax.ppermute(value, "seq", [(i, (i + by) % seq) for i in range(seq)])

    def mirror(value):
        pairs = []
        for i in range(seq):
            pairs.append((i, (i + 1) % seq))
            pairs.append((seq + i, seq + (i - 1) % seq))
        return lax.ppermute(value, ("groups", "seq"), pairs)

    def flip(value, axis):
        return lax.ppermute(value, axis, swap)

    def mod(value):
        return lax.rem(value + 2 * seq, seq)

    def columns(value, at, count):
        return lax.dynamic_slice_in_dim(value, at * count, count, 1)

    near_to = mod(z + 1 - 2 * y)
    near_of = mod(z - 1 + 2 * y)
    far_of = mod(z + 1 - 2 * y)
    across_of = mod(z + 2)

    w_near = mirror(columns(qkv_image, near_to, across))
    half = slab // 2
    w_half = shift(
        lax.dynamic_slice(qkv_image, (y * half, mod(z + 2) * across), (half, across)), 2
    )
    w_own = columns(qkv_image, z, across)

    quarter_rows = image_count // lanes
    quarter = lax.dynamic_slice_in_dim(image_tokens, q * quarter_rows, quarter_rows, 0)
    t1 = shift(quarter, 1)
    t3 = shift(quarter, -1)
    t2 = shift(t1, 1)
    w_far = flip(w_near, "groups")
    w_other = flip(w_half, "groups")

    text_slabs = [columns(text_tokens, z, slab)] + [
        shift(columns(text_tokens, mod(z + k), slab), k) for k in range(1, seq)
    ]

    embedded = lax.dynamic_index_in_dim(time_table, timestep[0], 0, keepdims=False).astype(
        jnp.float32
    )
    vector = jax.nn.silu(embedded).astype(jnp.bfloat16)
    vector_rows = lax.dynamic_slice_in_dim(vector, z * slab, slab)
    partial = mm(vector_rows[None, :], mod_weight)
    text_values = text_tokens.astype(jnp.float32)
    center = jnp.mean(text_values, axis=-1)
    spread = jnp.mean(jnp.square(text_values - center[:, None]), axis=-1)
    message = jnp.concatenate(
        [partial, center[None, :], lax.rsqrt(spread + EPSILON)[None, :]], axis=1
    )
    messages = [message] + [shift(message, k) for k in range(1, seq)]
    mine = partial.shape[1]
    summed = messages[0][:, :mine]
    for k in range(1, seq):
        summed = summed + messages[k][:, :mine]
    beside = flip(summed, "tensor")
    pair = jnp.concatenate([summed, beside], axis=0)
    other_pair = flip(pair, "sub")
    grid = jnp.stack([pair, other_pair], axis=1)
    grid = jnp.where(x == 1, grid[::-1], grid)
    grid = jnp.where(c == 1, grid[:, ::-1], grid)
    modulation = grid.reshape(2, 3, width)

    def absolute(parts):
        joined = jnp.concatenate([parts[0]] + parts[:0:-1], axis=0)
        return jnp.roll(joined, z * parts[0].shape[0], axis=0)

    stats = absolute([m[:, mine:].reshape(2, text_count).T for m in messages])
    text_all = absolute(text_slabs).astype(jnp.float32)
    text_mod = lax.dynamic_slice_in_dim(modulation[1, :2], z * slab, slab, 1)
    hidden_text = (
        (text_all - stats[:, :1]) * stats[:, 1:] * (1.0 + text_mod[1]) + text_mod[0]
    ).astype(jnp.bfloat16)
    text_partial = mm(hidden_text, qkv_text)
    text_parts = [columns(text_partial, z, across)] + [
        shift(columns(text_partial, mod(z + k), across).astype(jnp.bfloat16), k)
        for k in range(1, seq)
    ]

    gains = lax.dynamic_slice_in_dim(norm_gain, z, 1, 2)[:, :, 0]
    index = jnp.stack(
        [q, q ^ 2, q ^ 1, q ^ 3, z, near_of, far_of, across_of, y, 1 - y]
    ).astype(jnp.int32)
    weights = (w_own, w_near, w_far, w_half, w_other)
    vectors = (modulation[0, 1:2], modulation[0, 0:1], gains[0])

    def project(pieces):
        count = len(pieces)
        return pl.pallas_call(
            functools.partial(qkv_kernel, count),
            out_shape=jax.ShapeDtypeStruct((image_count, across), jnp.bfloat16),
            in_specs=[SMEM] + [VMEM] * (count + 8),
            out_specs=VMEM,
            scratch_shapes=[pltpu.VMEM((image_count, width), jnp.bfloat16)],
            name="qkv",
        )(index, *pieces, *weights, *vectors)

    blocks = [project([image_tokens])]
    for block in (t1, t2, t3):
        beside = flip(block, "tensor")
        blocks.append(project([block, beside, flip(block, "sub"), flip(beside, "sub")]))

    count = seq * image_count
    text_total = seq * text_count
    joint = (count + text_total, size)
    image_heads, text_heads = pl.pallas_call(
        functools.partial(attend_kernel, seq),
        out_shape=(
            jax.ShapeDtypeStruct((seq, image_count, size), jnp.bfloat16),
            jax.ShapeDtypeStruct((text_total, size), jnp.bfloat16),
        ),
        in_specs=[SMEM] + [VMEM] * (2 * seq + 1),
        out_specs=(VMEM, VMEM),
        scratch_shapes=[pltpu.VMEM(joint, jnp.bfloat16)] * 3,
        name="attend",
    )(text_length, *blocks, *text_parts, gains[1])

    p_near = mirror(proj_image)
    p_depth = proj_image.shape[0] // 2
    p_half = mirror(lax.dynamic_slice_in_dim(p_near, y * p_depth, p_depth, 0))
    p_far = flip(p_near, "groups")
    p_other = flip(p_half, "groups")

    returned = [image_heads[0]] + [shift(image_heads[k], -k) for k in range(1, seq)]
    gathered = [text_heads] + [shift(text_heads, k) for k in range(1, seq)]

    def slot(column):
        return jnp.where(column % sub == c, 2, 0) + jnp.where(column // sub == x, 1, 0)

    places = jnp.stack(
        [z, mod(z + 1), mod(z + 2), mod(z + 3)]
        + [slot(v) for v in (z, near_of, far_of, across_of)]
        + [y, 1 - y]
    ).astype(jnp.int32)
    piece = proj_image.shape[1]
    sums = pl.pallas_call(
        functools.partial(project_kernel, seq),
        out_shape=jax.ShapeDtypeStruct((lanes, image_count, piece), jnp.bfloat16),
        in_specs=[SMEM] + [VMEM] * (seq + 5),
        out_specs=VMEM,
        scratch_shapes=[pltpu.VMEM((image_count, seq * size), jnp.bfloat16)],
        name="project",
    )(places, *returned, proj_image, p_near, p_far, p_half, p_other)
    taken = flip(sums[:2], "sub").astype(jnp.float32)
    kept = sums[2:].astype(jnp.float32)
    sent = (kept[0] + taken[0]).astype(jnp.bfloat16)
    image_branch = kept[1] + taken[1] + flip(sent, "tensor").astype(jnp.float32)

    text_joined = jnp.concatenate([gathered[0]] + gathered[:0:-1], axis=1)
    text_joined = jnp.roll(text_joined, z * size, axis=1)
    text_sums = mm(text_joined, proj_text).astype(jnp.bfloat16)
    text_branch = jnp.zeros((text_count, piece), jnp.float32)
    for j in range(lanes):
        pairs = [
            (s * lanes + l, ((l + j) % lanes) * lanes + s) for s in range(seq) for l in range(lanes)
        ]
        rows = lax.dynamic_slice_in_dim(text_sums, lax.rem(q + j, lanes) * text_count, text_count, 0)
        text_branch += lax.ppermute(rows, ("seq", "tensor", "sub"), pairs).astype(jnp.float32)

    gates = lax.dynamic_slice_in_dim(modulation[:, 2], q * piece, piece, 1)
    image_base = columns(image_tokens, q, piece).astype(jnp.float32)
    text_base = columns(text_tokens, q, piece).astype(jnp.float32)
    image_out = (image_base + gates[0] * image_branch).astype(jnp.bfloat16)
    text_out = (text_base + gates[1] * text_branch).astype(jnp.bfloat16)
    return (image_out, text_out)


def split_heads(projected, gains):
    shaped = projected.reshape(projected.shape[0], -1, 3, gains.shape[-1])
    queries = head_norm(shaped[:, :, 0], gains[0]).astype(jnp.bfloat16)
    keys = head_norm(shaped[:, :, 1], gains[1]).astype(jnp.bfloat16)
    values = shaped[:, :, 2].astype(jnp.bfloat16)
    return (queries, keys, values)


def add_rows(source, shards):
    return jnp.dot(source, shards, preferred_element_type=jnp.float32)


def body(
    image_tokens,
    text_tokens,
    timestep,
    text_length,
    time_table,
    mod_weight,
    qkv_image,
    qkv_text,
    norm_gain,
    proj_image,
    proj_text,
):
    columns_all = image_tokens.shape[1]
    embedded = lax.dynamic_index_in_dim(time_table, timestep[0], 0, keepdims=False).astype(
        jnp.float32
    )
    vector = jax.nn.silu(embedded).astype(jnp.bfloat16)
    slab_rows = mod_weight.shape[0]
    vector_rows = lax.dynamic_slice_in_dim(vector, lax.axis_index("seq") * slab_rows, slab_rows)
    partial_value = jnp.dot(vector_rows[None, :], mod_weight, preferred_element_type=jnp.float32)[0]
    summed_rows = lax.psum(partial_value, "seq")
    modulation = lax.all_gather(summed_rows, ("tensor", "sub"), axis=0, tiled=True)
    modulation = modulation.reshape(2, 3, columns_all)
    hidden_image = modulate(image_tokens, modulation[0, 0], modulation[0, 1])
    hidden_text = modulate(text_tokens, modulation[1, 0], modulation[1, 1])
    image_count = image_tokens.shape[0]
    text_count = text_tokens.shape[0]
    local_rows = image_count + text_count
    projected_image = add_rows(hidden_image, lax.all_gather(qkv_image, "seq", axis=0, tiled=True))
    projected_text = add_rows(hidden_text, lax.all_gather(qkv_text, "seq", axis=0, tiled=True))
    image_q, image_k, image_v = split_heads(projected_image, norm_gain[0])
    text_q, text_k, text_v = split_heads(projected_text, norm_gain[1])
    heads_here = image_q.shape[1]
    head_size = image_q.shape[2]
    queries = jnp.concatenate([text_q, image_q], axis=0)
    keys = jnp.concatenate([text_k, image_k], axis=0)
    values = jnp.concatenate([text_v, image_v], axis=0)
    keys_values = jnp.stack([keys, values], axis=2).reshape(local_rows, heads_here * 2 * head_size)
    factor = float(head_size) ** (-0.5)
    shards = lax.all_gather(keys_values, "seq", axis=0, tiled=True)
    count = shards.shape[0]
    blocks = shards.reshape(count, heads_here, 2, head_size)
    position = jnp.arange(count, dtype=jnp.int32)
    within = position % local_rows
    owner = position // local_rows
    usable = (within >= text_count) | (owner * text_count + within < text_length[0])
    scores = (
        jnp.einsum("qhd,khd->hqk", queries, blocks[:, :, 0], preferred_element_type=jnp.float32)
        * factor
    )
    scores = jnp.where(usable[None, None, :], scores, -1e30)
    run_max = jnp.full((heads_here, local_rows), -1e30, jnp.float32)
    new_max = jnp.maximum(run_max, jnp.max(scores, axis=-1))
    probs = jnp.exp(scores - new_max[:, :, None])
    run_sum = jnp.sum(probs, axis=-1)
    totals = jnp.einsum(
        "hqk,khd->hqd",
        probs.astype(jnp.bfloat16),
        blocks[:, :, 1],
        preferred_element_type=jnp.float32,
    )
    final_max, run_sum, totals = (new_max, run_sum, totals)
    attended = (
        (totals / run_sum[:, :, None])
        .astype(jnp.bfloat16)
        .transpose(1, 0, 2)
        .reshape(local_rows, heads_here * head_size)
    )
    stacked = jnp.stack([proj_image, proj_text], axis=0)
    text_attended = attended[:text_count]
    image_attended = attended[text_count:]
    shards = lax.all_gather(stacked, "seq", axis=2, tiled=True)
    text_part = jnp.dot(text_attended, shards[1], preferred_element_type=jnp.float32)
    image_part = jnp.dot(image_attended, shards[0], preferred_element_type=jnp.float32)
    branch = jnp.concatenate([text_part, image_part], axis=0)
    summed = lax.psum_scatter(
        branch.astype(jnp.bfloat16), ("tensor", "sub"), scatter_dimension=1, tiled=True
    ).astype(jnp.float32)
    width_here = summed.shape[1]
    first = lax.axis_index(("tensor", "sub")) * width_here
    gates = lax.dynamic_slice_in_dim(modulation[:, 2], first, width_here, 1)
    image_base = lax.dynamic_slice_in_dim(image_tokens, first, width_here, 1).astype(jnp.float32)
    text_base = lax.dynamic_slice_in_dim(text_tokens, first, width_here, 1).astype(jnp.float32)
    image_out = (image_base + gates[0] * summed[text_count:]).astype(jnp.bfloat16)
    text_out = (text_base + gates[1] * summed[:text_count]).astype(jnp.bfloat16)
    return (image_out, text_out)


def solution(mesh):
    shape = mesh.shape

    def program(*args):
        seq, lanes = lax.axis_size("seq"), lax.axis_size("tensor") * lax.axis_size("sub")
        heads_here = args[8].shape[2]
        square = seq == lanes == heads_here == 4
        pairs = all(shape[name] == 2 for name in ("groups", "tensor", "sub"))
        return (split_body if square and pairs else body)(*args)

    return jax.shard_map(
        program,
        mesh=mesh,
        in_specs=(
            P(("groups", "seq"), None),
            P(("groups", "seq"), None),
            P("groups"),
            P("groups"),
            P(),
            P("seq", ("tensor", "sub")),
            P("seq", ("tensor", "sub")),
            P("seq", ("tensor", "sub")),
            P(None, None, ("tensor", "sub"), None),
            P(("tensor", "sub"), "seq"),
            P(("tensor", "sub"), "seq"),
        ),
        out_specs=(
            P(("groups", "seq"), ("tensor", "sub")),
            P(("groups", "seq"), ("tensor", "sub")),
        ),
        check_vma=False,
    )
```
